32 devices in a mesh: blk: 32 (over z, y, x, core).
Axes of the slice: x: 2, y: 2, z: 4, core: 2. Of those that a mesh axis runs over, the one named last changes fastest.
Arguments:
- geometry: float32 [8, 32768], P(None, 'blk'), may hold values from -1 to 9.333333, as said below
- currents: float32 [32, 32768], P(None, 'blk'), may hold values from -6 to 6
- net_ids: int32 [32768], P('blk'), may hold values from 0 to 3
- pair_on: int32 [32, 8], P('blk'), may hold values from 0 to 1, as said below
Outputs:
- voltage: float32 [32, 32768], P(None, 'blk')
The draws below stay inside these ranges and needn't reach their ends.
Inputs may be any that keep to these rules, and one draw needn't show every extreme that they name: `geometry`: rows 0 to 1 lie in 0 to 32 / 6 + 4, row 2 in 0 to 0.2, rows 3 to 5 form a unit vector, row 6 lies in 0.2 to 2 and row 7 in 0.05 to 0.5. Symmetric: pair_on[b, 4 + d - 1] equals pair_on[(b + d) mod 32, d - 1] for d = 1 .. 4.
All inputs are finite; a program needn't handle non-finite values.
Results may differ from the reference program's by a relative error of at most 0.0003.
Values sent between devices are 32-bit elements; how exact they have to be, the bound alone decides.
A program may use at most 64 MiB of HBM per device.

```python
import jax
import jax.numpy as jnp
from jax import lax

SEG_DEV = 1024
COLS = 32
REACH = 4
NETS = 4
SEGMENTS = 32768
N_BLK = 32


def draw_geometry(key, part):
    keys = jax.random.split(jax.random.fold_in(key, 11), 7)
    count = SEGMENTS
    spacing = 0.5
    loop_radius = N_BLK * spacing / (2.0 * jnp.pi)
    block_index = (jnp.arange(count, dtype=jnp.int32) // SEG_DEV).astype(jnp.float32)
    theta = 2.0 * jnp.pi * block_index / N_BLK
    centre_x = 2.0 + loop_radius + loop_radius * jnp.cos(theta)
    centre_y = 2.0 + loop_radius + loop_radius * jnp.sin(theta)
    spread = jax.random.uniform(keys[0], (2, count), jnp.float32, -1.25, 1.25)
    height = jax.random.uniform(keys[1], (1, count), jnp.float32, 0.0, 0.2)
    centres = jnp.concatenate([(centre_x + spread[0])[None, :], (centre_y + spread[1])[None, :], height], axis=0)
    along_y = jax.random.randint(keys[2], (count,), 0, 2).astype(jnp.float32)
    sign = 2.0 * jax.random.randint(keys[3], (count,), 0, 2).astype(jnp.float32) - 1.0
    tilt = 0.3 * jax.random.normal(keys[4], (3, count), jnp.float32)
    raw_dir = jnp.stack([sign * (1.0 - along_y) + tilt[0], sign * along_y + tilt[1], 0.3 * tilt[2]])
    direction = raw_dir / jnp.sqrt(jnp.sum(raw_dir * raw_dir, axis=0, keepdims=True))
    length = jnp.exp(jax.random.uniform(keys[5], (1, count), jnp.float32, jnp.log(0.2), jnp.log(2.0)))
    radius = jnp.exp(jax.random.uniform(keys[6], (1, count), jnp.float32, jnp.log(0.05), jnp.log(0.5)))
    return jnp.concatenate([centres, direction, length, radius], axis=0).astype(jnp.float32)


def draw_pair_on(key, part):
    base = jax.random.randint(jax.random.fold_in(key, 23), (N_BLK, REACH), 0, 4)
    marks = (base > 0).astype(jnp.int32)
    lower = [jnp.roll(marks[:, k], k + 1) for k in range(REACH)]
    upper = [marks[:, k] for k in range(REACH)]
    return jnp.stack(lower + upper, axis=1).astype(jnp.int32)


def plant(values, own_key, least, high):
    dims = values.shape
    place = [jax.random.randint(jax.random.fold_in(own_key, axis), (), 0, dims[axis]) for axis in range(len(dims))]
    values = values.at[tuple(place)].set(least)
    longest = dims.index(max(dims))
    place[longest] = (place[longest] + 1) % dims[longest]
    return values.at[tuple(place)].set(high)


def shard_levels(rng, dims, pieces, low, largest):
    factor_of = 1.0
    for dim, parts in pieces:
        heights = jax.random.uniform(jax.random.fold_in(jax.random.fold_in(rng, 6), dim), (parts,), jnp.float32, low / len(pieces), largest / len(pieces))
        factor_of = factor_of * jnp.repeat(jnp.exp(heights), dims[dim] // parts).reshape((-1,) + (1,) * (len(dims) - 1 - dim))
    return factor_of


def centred(stream_key, extent, scale, limit, shards=(), kind=jnp.bfloat16):
    level = shard_levels(stream_key, extent, shards, -0.22, 0.18) if shards else 1.0
    array = jax.random.normal(stream_key, extent, jnp.float32) * scale * level
    return jnp.minimum(jnp.maximum(array, -limit), limit).astype(kind)


def setup_inputs(seed: int = 0) -> dict:
    splits = jax.random.split(jax.random.key(seed), 5)
    geometry = draw_geometry(jax.random.fold_in(splits[4], 71), 0)
    currents = centred(splits[1], (COLS, SEGMENTS), 1.0, 6.0, ((1, 32),), jnp.float32)
    net_ids = plant(jax.random.randint(splits[2], (SEGMENTS,), 0, NETS), jax.random.fold_in(splits[2], 1), 0, NETS - 1).astype(jnp.int32)
    pair_on = draw_pair_on(jax.random.fold_in(splits[4], 71), 0)
    return dict(geometry=geometry, currents=currents, net_ids=net_ids, pair_on=pair_on)


def kernel_tile(own, other):
    delta_x = own[0][:, None] - other[0][None, :]
    delta_y = own[1][:, None] - other[1][None, :]
    delta_z = own[2][:, None] - other[2][None, :]
    dist_sq = delta_x * delta_x + delta_y * delta_y + delta_z * delta_z
    radius_sq = (own[7] * own[7])[:, None] + (other[7] * other[7])[None, :]
    cosine = own[3][:, None] * other[3][None, :] + own[4][:, None] * other[4][None, :] + own[5][:, None] * other[5][None, :]
    lengths = own[6][:, None] * other[6][None, :]
    netf = jnp.where(own[8][:, None] == other[8][None, :], jnp.float32(1.0), jnp.float32(0.5))
    return cosine * lengths * netf * 0.1 / jnp.sqrt(dist_sq + radius_sq)

def apply_tile(own, other):
    tile = kernel_tile(own, other)
    return lax.dot_general(other[9:], tile, (((1,), (1,)), ((), ())), precision=lax.Precision.HIGHEST, preferred_element_type=jnp.float32)

def reference(geometry, currents, net_ids, pair_on):
    packed = jnp.concatenate([geometry, net_ids.astype(jnp.float32)[None, :], currents], axis=0)
    rows_all = packed.shape[0]
    blocks = packed.reshape(rows_all, N_BLK, SEG_DEV).transpose(1, 0, 2)
    offsets = [-(k + 1) for k in range(REACH)] + [k + 1 for k in range(REACH)]

    def one_block(index):
        own = lax.dynamic_index_in_dim(blocks, index, 0, keepdims=False)
        total = apply_tile(own, own)
        for position, offset in enumerate(offsets):
            where = ((index + offset) % N_BLK).astype(jnp.int32)
            other = lax.dynamic_index_in_dim(blocks, where, 0, keepdims=False)
            flag = lax.dynamic_index_in_dim(pair_on[:, position], index, 0, keepdims=False).astype(jnp.float32)
            total = total + flag * apply_tile(own, other)
        return total
    result = lax.map(one_block, jnp.arange(N_BLK, dtype=jnp.int32))
    return result.transpose(1, 0, 2).reshape(COLS, SEGMENTS)
```

```python
import functools

import jax
import jax.numpy as jnp
from jax import lax
from jax.experimental import pallas as pl
from jax.experimental.pallas import tpu as pltpu
from jax.sharding import PartitionSpec as P

MESH = pl.DeviceIdType.MESH
NETS = 4
GEO = 8
FEATURES = 128
GEO_AT = 112
CHUNK = 256
LANES = 256
F32 = jnp.float32
BF16 = jnp.bfloat16


def rounded(x):
    return x.astype(BF16).astype(F32)


def split(x):
    high = rounded(x)
    return high, rounded(x - high)


def split3(x):
    high = rounded(x)
    mid = rounded(x - high)
    return high, mid, rounded(x - high - mid)


def stack_rows(rows, wide):
    at = lax.broadcasted_iota(jnp.int32, (GEO, wide), 0)
    tiles = []
    for first in range(0, len(rows), GEO):
        tile = jnp.zeros((GEO, wide), F32)
        for k, row in enumerate(rows[first : first + GEO]):
            tile = jnp.where(at == k, row, tile)
        tiles.append(tile)
    return tiles


def other_features(geo, net):
    wide = geo.shape[1]
    scaled = geo * geo[6:7]
    highs, lows = [], []
    for n in range(NETS):
        high, low = split(scaled * jnp.where(net == n, F32(1.0), F32(0.5)))
        highs.append(high)
        lows.append(low)
    z, r = geo[2:3], geo[7:8]
    one = jnp.ones_like(z)
    ah, am, al = split3(z * z + r * r)
    zh, zm, zl = split3(z)
    near = stack_rows([ah, am, al, one, one, one, zh, zh, zh, zm, zm, zl], wide)
    pad = jnp.zeros((GEO, wide), F32)
    return jnp.concatenate(highs + lows + highs + near + [geo, pad], axis=0)


def own_features(geo, net):
    wide = geo.shape[1]
    at = lax.broadcasted_iota(jnp.int32, (GEO, wide), 0)
    scaled = jnp.where((at >= 3) & (at < 6), geo * (geo[6:7] * F32(0.1)), F32(0.0))
    highs, lows = [], []
    for n in range(NETS):
        high, low = split(jnp.where(net == n, scaled, F32(0.0)))
        highs.append(high)
        lows.append(low)
    z, r = geo[2:3], geo[7:8]
    one = jnp.ones_like(z)
    ah, am, al = split3(z * z + r * r)
    zh, zm, zl = (F32(-2.0) * part for part in split3(z))
    near = stack_rows([one, one, one, ah, am, al, zh, zm, zl, zh, zm, zh], wide)
    pad = jnp.zeros((GEO, wide), F32)
    product = jnp.concatenate(highs + highs + lows + [pad] * 4, axis=0)
    radial = jnp.concatenate([pad] * (3 * NETS) + near + [pad] * 2, axis=0)
    return product.astype(BF16), radial.astype(BF16)


def body(n, reach, geo, cur, net, pair, out, geo_in, cur_in, net_in, product, radial, send_sem, recv_sem):
    me = lax.axis_index("blk")
    seg = geo.shape[1]
    cols = cur.shape[0]
    offsets = [-(k + 1) for k in range(reach)] + [k + 1 for k in range(reach)]

    barrier = pltpu.get_barrier_semaphore()
    for o in offsets:
        pl.semaphore_signal(barrier, inc=1, device_id=(lax.rem(me + o + n, n),), device_id_type=MESH)
    pl.semaphore_wait(barrier, len(offsets))

    copies = {}
    order = [k for d in range(reach) for k in (d, reach + d)]
    for k in order:
        target = lax.rem(me - offsets[k] + n, n)
        for part, (src, dst) in enumerate(((geo, geo_in), (net, net_in), (cur, cur_in))):
            copy = pltpu.make_async_remote_copy(
                src_ref=src,
                dst_ref=dst.at[k],
                send_sem=send_sem.at[k, part],
                recv_sem=recv_sem.at[k, part],
                device_id=(target,),
                device_id_type=MESH,
            )
            copy.start()
            copies[k, part] = copy

    for first in range(0, seg, LANES):
        at = pl.ds(first, LANES)
        product[:, at], radial[:, at] = own_features(geo[:, at], net[:, at])
    out[...] = jnp.zeros_like(out)

    def tile(geo_o, cur_o, net_o, flag):
        @pl.loop(0, seg // CHUNK)
        def _(c):
            at = pl.ds(pl.multiple_of(c * CHUNK, CHUNK), CHUNK)
            feats = other_features(geo_o[:, at], net_o[:, at]).T
            low_feats = feats.astype(BF16)
            x_o = feats[:, GEO_AT : GEO_AT + 1]
            y_o = feats[:, GEO_AT + 1 : GEO_AT + 2]
            data = cur_o[:, at]
            if flag is not None:
                data = data * flag
            high = data.astype(BF16)
            both = jnp.concatenate([high, (data - high.astype(F32)).astype(BF16)], axis=0)
            for first in range(0, seg, LANES):
                own = pl.ds(first, LANES)
                g = jnp.dot(low_feats, product[:, own], preferred_element_type=F32)
                near = jnp.dot(low_feats, radial[:, own], preferred_element_type=F32)
                dx = geo[0:1, own] - x_o
                dy = geo[1:2, own] - y_o
                kern = g * lax.rsqrt(dx * dx + dy * dy + near)
                kh = kern.astype(BF16)
                kl = (kern - kh.astype(F32)).astype(BF16)
                v = jnp.dot(both, kh, preferred_element_type=F32) + jnp.dot(both, kl, preferred_element_type=F32)
                out[:, own] += v[:cols] + v[cols:]

    tile(geo, cur, net, None)

    per = lax.rem(me, 2 * reach)
    low_first = per >= reach

    @pl.loop(0, 2 * reach)
    def _(t):
        k = jnp.where(low_first, t, lax.rem(t + reach, 2 * reach))
        for part, (src, dst) in enumerate(((geo, geo_in), (net, net_in), (cur, cur_in))):
            pltpu.make_async_remote_copy(
                src_ref=src,
                dst_ref=dst.at[k],
                send_sem=send_sem.at[k, part],
                recv_sem=recv_sem.at[k, part],
                device_id=(lax.rem(me + 1, n),),
                device_id_type=MESH,
            ).wait_recv()
        flags = pair[...].astype(F32)
        lane = lax.broadcasted_iota(jnp.int32, flags.shape, 1)
        flag = jnp.sum(jnp.where(lane == k, flags, F32(0.0)), axis=1, keepdims=True)
        tile(geo_in.at[k], cur_in.at[k], net_in.at[k], flag)

    for copy in copies.values():
        copy.wait_send()


def shards(n, geometry, currents, net_ids, pair_on):
    reach = pair_on.shape[1] // 2
    seg = geometry.shape[1]
    cols = currents.shape[0]
    near = 2 * reach
    vmem = pl.BlockSpec(memory_space=pltpu.VMEM)
    return pl.pallas_call(
        functools.partial(body, n, reach),
        out_shape=jax.ShapeDtypeStruct((cols, seg), F32),
        in_specs=[vmem] * 4,
        out_specs=vmem,
        scratch_shapes=[
            pltpu.VMEM((near, GEO, seg), F32),
            pltpu.VMEM((near, cols, seg), F32),
            pltpu.VMEM((near, 1, seg), jnp.int32),
            pltpu.VMEM((FEATURES, seg), BF16),
            pltpu.VMEM((FEATURES, seg), BF16),
            pltpu.SemaphoreType.DMA((near, 3)),
            pltpu.SemaphoreType.DMA((near, 3)),
        ],
        compiler_params=pltpu.CompilerParams(collective_id=0, has_side_effects=True),
    )(geometry, currents, net_ids[None, :], pair_on)


def solution(mesh):
    return jax.shard_map(
        functools.partial(shards, mesh.shape["blk"]),
        mesh=mesh,
        in_specs=(P(None, "blk"), P(None, "blk"), P("blk"), P("blk", None)),
        out_specs=P(None, "blk"),
        check_vma=False,
    )
```

```python
import functools

import jax
import jax.numpy as jnp
from jax import lax
from jax.experimental import pallas as pl
from jax.experimental.pallas import tpu as pltpu
from jax.sharding import PartitionSpec as P

MESH = pl.DeviceIdType.MESH
NETS = 4
GEO = 8
FEATURES = 128
GEO_AT = 112
CHUNK = 256
LANES = 1024
F32 = jnp.float32
BF16 = jnp.bfloat16


def rounded(x):
    return x.astype(BF16).astype(F32)


def split(x):
    high = rounded(x)
    return high, rounded(x - high)


def split3(x):
    high = rounded(x)
    mid = rounded(x - high)
    return high, mid, rounded(x - high - mid)


def stack_rows(rows, wide):
    at = lax.broadcasted_iota(jnp.int32, (GEO, wide), 0)
    tiles = []
    for first in range(0, len(rows), GEO):
        tile = jnp.zeros((GEO, wide), F32)
        for k, row in enumerate(rows[first : first + GEO]):
            tile = jnp.where(at == k, row, tile)
        tiles.append(tile)
    return tiles


def other_features(geo, net):
    wide = geo.shape[1]
    scaled = geo * geo[6:7]
    highs, lows = [], []
    for n in range(NETS):
        high, low = split(scaled * jnp.where(net == n, F32(1.0), F32(0.5)))
        highs.append(high)
        lows.append(low)
    z, r = geo[2:3], geo[7:8]
    one = jnp.ones_like(z)
    ah, am, al = split3(z * z + r * r)
    zh, zm, zl = split3(z)
    near = stack_rows([ah, am, al, one, one, one, zh, zh, zh, zm, zm, zl], wide)
    pad = jnp.zeros((GEO, wide), F32)
    return jnp.concatenate(highs + lows + highs + near + [geo, pad], axis=0)


def own_features(geo, net):
    wide = geo.shape[1]
    at = lax.broadcasted_iota(jnp.int32, (GEO, wide), 0)
    scaled = jnp.where((at >= 3) & (at < 6), geo * (geo[6:7] * F32(0.1)), F32(0.0))
    highs, lows = [], []
    for n in range(NETS):
        high, low = split(jnp.where(net == n, scaled, F32(0.0)))
        highs.append(high)
        lows.append(low)
    z, r = geo[2:3], geo[7:8]
    one = jnp.ones_like(z)
    ah, am, al = split3(z * z + r * r)
    zh, zm, zl = (F32(-2.0) * part for part in split3(z))
    near = stack_rows([one, one, one, ah, am, al, zh, zm, zl, zh, zm, zh], wide)
    pad = jnp.zeros((GEO, wide), F32)
    product = jnp.concatenate(highs + highs + lows + [pad] * 4, axis=0)
    radial = jnp.concatenate([pad] * (3 * NETS) + near + [pad] * 2, axis=0)
    return product.astype(BF16), radial.astype(BF16)


def body(n, reach, geo, cur, net, pair, out, geo_in, cur_in, net_in, product, radial, send_sem, recv_sem):
    me = lax.axis_index("blk")
    seg = geo.shape[1]
    cols = cur.shape[0]
    offsets = [-(k + 1) for k in range(reach)] + [k + 1 for k in range(reach)]

    barrier = pltpu.get_barrier_semaphore()
    for o in offsets:
        pl.semaphore_signal(barrier, inc=1, device_id=(lax.rem(me + o + n, n),), device_id_type=MESH)
    pl.semaphore_wait(barrier, len(offsets))

    copies = {}
    order = [k for d in range(reach) for k in (d, reach + d)]
    for k in order:
        target = lax.rem(me - offsets[k] + n, n)
        for part, (src, dst) in enumerate(((geo, geo_in), (net, net_in), (cur, cur_in))):
            copy = pltpu.make_async_remote_copy(
                src_ref=src,
                dst_ref=dst.at[k],
                send_sem=send_sem.at[k, part],
                recv_sem=recv_sem.at[k, part],
                device_id=(target,),
                device_id_type=MESH,
            )
            copy.start()
            copies[k, part] = copy

    for first in range(0, seg, LANES):
        at = pl.ds(first, LANES)
        product[:, at], radial[:, at] = own_features(geo[:, at], net[:, at])
    out[...] = jnp.zeros_like(out)

    def tile(geo_o, cur_o, net_o, flag):
        @pl.loop(0, seg // CHUNK)
        def _(c):
            at = pl.ds(pl.multiple_of(c * CHUNK, CHUNK), CHUNK)
            feats = other_features(geo_o[:, at], net_o[:, at]).T
            low_feats = feats.astype(BF16)
            x_o = feats[:, GEO_AT : GEO_AT + 1]
            y_o = feats[:, GEO_AT + 1 : GEO_AT + 2]
            z_o = feats[:, GEO_AT + 2 : GEO_AT + 3]
            r_o = feats[:, GEO_AT + 7 : GEO_AT + 8]
            a_o = z_o * z_o + r_o * r_o
            z_o = z_o + z_o
            data = cur_o[:, at]
            if flag is not None:
                data = data * flag
            high = data.astype(BF16)
            both = jnp.concatenate([high, (data - high.astype(F32)).astype(BF16)], axis=0)
            for first in range(0, seg, LANES):
                own = pl.ds(first, LANES)
                g = jnp.dot(low_feats, product[:, own], preferred_element_type=F32)
                a_i = geo[2:3, own] * geo[2:3, own] + geo[7:8, own] * geo[7:8, own]
                near = (a_i + a_o) - geo[2:3, own] * z_o
                dx = geo[0:1, own] - x_o
                dy = geo[1:2, own] - y_o
                kern = g * lax.rsqrt(dx * dx + dy * dy + near)
                kh = kern.astype(BF16)
                kl = (kern - kh.astype(F32)).astype(BF16)
                v = jnp.dot(both, kh, preferred_element_type=F32) + jnp.dot(both, kl, preferred_element_type=F32)
                out[:, own] += v[:cols] + v[cols:]

    tile(geo, cur, net, None)

    per = lax.rem(me, 2 * reach)
    low_first = per >= reach

    @pl.loop(0, 2 * reach)
    def _(t):
        k = jnp.where(low_first, t, lax.rem(t + reach, 2 * reach))
        for part, (src, dst) in enumerate(((geo, geo_in), (net, net_in), (cur, cur_in))):
            pltpu.make_async_remote_copy(
                src_ref=src,
                dst_ref=dst.at[k],
                send_sem=send_sem.at[k, part],
                recv_sem=recv_sem.at[k, part],
                device_id=(lax.rem(me + 1, n),),
                device_id_type=MESH,
            ).wait_recv()
        flags = pair[...].astype(F32)
        lane = lax.broadcasted_iota(jnp.int32, flags.shape, 1)
        flag = jnp.sum(jnp.where(lane == k, flags, F32(0.0)), axis=1, keepdims=True)
        tile(geo_in.at[k], cur_in.at[k], net_in.at[k], flag)

    for copy in copies.values():
        copy.wait_send()


def shards(n, geometry, currents, net_ids, pair_on):
    reach = pair_on.shape[1] // 2
    seg = geometry.shape[1]
    cols = currents.shape[0]
    near = 2 * reach
    vmem = pl.BlockSpec(memory_space=pltpu.VMEM)
    return pl.pallas_call(
        functools.partial(body, n, reach),
        out_shape=jax.ShapeDtypeStruct((cols, seg), F32),
        in_specs=[vmem] * 4,
        out_specs=vmem,
        scratch_shapes=[
            pltpu.VMEM((near, GEO, seg), F32),
            pltpu.VMEM((near, cols, seg), F32),
            pltpu.VMEM((near, 1, seg), jnp.int32),
            pltpu.VMEM((FEATURES, seg), BF16),
            pltpu.VMEM((FEATURES, seg), BF16),
            pltpu.SemaphoreType.DMA((near, 3)),
            pltpu.SemaphoreType.DMA((near, 3)),
        ],
        compiler_params=pltpu.CompilerParams(collective_id=0, has_side_effects=True),
    )(geometry, currents, net_ids[None, :], pair_on)


def solution(mesh):
    return jax.shard_map(
        functools.partial(shards, mesh.shape["blk"]),
        mesh=mesh,
        in_specs=(P(None, "blk"), P(None, "blk"), P("blk"), P("blk", None)),
        out_specs=P(None, "blk"),
        check_vma=False,
    )
```
